32 devices in a mesh: row: 16 (over z, x, core), col: 2 (over y).
Axes of the slice: x: 2, y: 2, z: 4, core: 2. Of those that a mesh axis runs over, the one named last changes fastest.
Arguments:
- tokens: bfloat16 [1024, 8192], P('row', 'col'), may hold values from -6 to 6
- norm_gain: bfloat16 [8192], P('col'), may hold values from 0.099609375 to 1.8984375
- gate_proj: bfloat16 [8192, 28672], P('col', 'row'), may hold values from -0.0625 to 0.0625
- up_proj: bfloat16 [8192, 28672], P('col', 'row'), may hold values from -0.0625 to 0.0625
- down_proj: bfloat16 [28672, 8192], P('row', 'col'), may hold values from -0.03125 to 0.03125
Outputs:
- mixed: bfloat16 [1024, 8192], P('row', 'col')
The draws below stay inside these ranges and needn't reach their ends.
All inputs are finite; a program needn't handle non-finite values.
Results may differ from the reference program's by a relative error of at most 0.015.
Values may be sent and summed in bfloat16 or wider, within the bound.
A program may use at most 128 MiB of HBM per device.

```python
import jax
import jax.numpy as jnp
from jax import lax

D = 8192
FF = 28672
TOKENS = 1024


def steps_of(own_key, extent, split, smallest, top_value):
    level = 1.0
    for position, blocks in split:
        draws = jax.random.uniform(jax.random.fold_in(jax.random.fold_in(own_key, 6), position), (blocks,), jnp.float32, smallest / len(split), top_value / len(split))
        level = level * jnp.repeat(jnp.exp(draws), extent[position] // blocks).reshape((-1,) + (1,) * (len(extent) - 1 - position))
    return level


def noise(stream_key, extent, width, limit, cuts=(), dtype=jnp.bfloat16):
    factor_of = steps_of(stream_key, extent, cuts, -0.22, 0.18) if cuts else 1.0
    array = jax.random.normal(stream_key, extent, jnp.float32) * width * factor_of
    return jnp.minimum(jnp.maximum(array, -limit), limit).astype(dtype)


def setup_inputs(seed: int = 0) -> dict:
    streams_of = jax.random.split(jax.random.key(seed), 6)
    tokens = noise(streams_of[0], (TOKENS, D), 1.0, 6.0, ((0, 16), (1, 2)))
    norm_gain = jnp.clip(1.0 + 0.18 * jax.random.normal(streams_of[1], (D,), jnp.float32), 0.099609375, 1.8984375).astype(jnp.bfloat16)
    gate_proj = noise(streams_of[2], (D, FF), D ** -0.5, 0.0625, ((0, 2), (1, 16)))
    up_proj = noise(streams_of[3], (D, FF), D ** -0.5, 0.0625, ((0, 2), (1, 16)))
    down_proj = noise(streams_of[4], (FF, D), FF ** -0.5, 0.03125, ((0, 16), (1, 2)))
    return {"tokens": tokens, "norm_gain": norm_gain, "gate_proj": gate_proj, "up_proj": up_proj, "down_proj": down_proj}


floor_term = 0.25

def reference(tokens, norm_gain, gate_proj, up_proj, down_proj):
    widened = tokens.astype(jnp.float32)
    square_sum = lax.optimization_barrier(jnp.sum(widened * widened, axis=1))
    row_scale = 1.0 / jnp.sqrt(square_sum / D + floor_term)
    scaled = (widened * norm_gain.astype(jnp.float32)[None, :]).astype(jnp.bfloat16)
    gate = row_scale[:, None] * jnp.dot(scaled, gate_proj, preferred_element_type=jnp.float32)
    up_value = row_scale[:, None] * jnp.dot(scaled, up_proj, preferred_element_type=jnp.float32)
    hidden = (jax.nn.silu(gate) * up_value).astype(jnp.bfloat16)
    mixed = widened + jnp.dot(hidden, down_proj, preferred_element_type=jnp.float32)
    return mixed.astype(jnp.bfloat16)
```

```python
import functools

import jax
import jax.numpy as jnp
from jax import lax
from jax.experimental import pallas as pl
from jax.experimental.pallas import tpu as pltpu
from jax.sharding import PartitionSpec as P

floor_term = 0.25
MESH = pl.DeviceIdType.MESH
BF = jnp.bfloat16
F32 = jnp.float32


def places(rows):
    n = rows // 2
    row, col = lax.axis_index("row"), lax.axis_index("col")
    core, chip = row % 2, row // 2
    z, x = chip // 2, chip % 2
    pos = z + x * (n - 1 - 2 * z)

    def at(p):
        p = (p + n) % n
        far = (2 * p) // n
        return ((1 - far) * 2 * p + far * (2 * (n - 1 - p) + 1)) * 2 + core

    right, left = (at(pos + 1), col), (at(pos - 1), col)
    return core, col, right, left, (row + 1 - 2 * core, col), (row, 1 - col)


def greet(partners):
    barrier = pltpu.get_barrier_semaphore()
    for device in partners:
        pl.semaphore_signal(barrier, inc=1, device_id=device, device_id_type=MESH)
    return lambda: pl.semaphore_wait(barrier, len(partners))


def remote(src, dst, send, recv, device):
    return pltpu.make_async_remote_copy(
        src_ref=src, dst_ref=dst, send_sem=send, recv_sem=recv, device_id=device, device_id_type=MESH
    )


def fused_kernel(rows, cols, tile, lead, tok_hbm, gain, wg_hbm, wu_hbm, wd_hbm, out, wg, wu, wd, x, pb, rv, pd, kept, sq, sq_in, sc,
                 tok_sem, wg_sem, wu_sem, wd_sem, sq_sem, ring_s, ring_r, sib_s, sib_r, lead_s, lead_r, y_s, y_r,
                 ds_s, ds_r, rs_s, rs_r, sc_s, sc_r, free):
    n = rows // 2
    half, width = out.shape[0] // 2, out.shape[1]
    units = wg.shape[1]
    leads = units // lead
    keep = pb.shape[0]
    parts, piece = pd.shape[1], pd.shape[5]
    core, col, right, left, sibling, across = places(rows)
    load_tok = pltpu.make_async_copy(tok_hbm, out, tok_sem)
    load_d = pltpu.make_async_copy(wd_hbm, wd, wd_sem)

    def lead_cols(t):
        return pl.ds(pl.multiple_of(t * lead, lead), lead)

    def load_g(t):
        return pltpu.make_async_copy(wg_hbm.at[:, lead_cols(t)], wg.at[:, lead_cols(t)], wg_sem.at[t])

    def load_u(t):
        return pltpu.make_async_copy(wu_hbm.at[:, lead_cols(t)], wu.at[:, lead_cols(t)], wu_sem.at[t])

    def scale_ring(s):
        onward = (jnp.where(col == 0, right[0], left[0]), col)
        return remote(sc.at[s, core], sc.at[s + 1, core], sc_s.at[s, 0], sc_r.at[s, 0], onward)

    def scale_sib(s):
        return remote(sc.at[s, core], sc.at[s, core], sc_s.at[s, 1], sc_r.at[s, 1], sibling)

    def scale_on(s):
        scale_sib(s).start()

        @pl.when(s < n - 1)
        def _():
            scale_ring(s).start()

    def ring(s, d):
        return remote(x.at[s, d, core], x.at[s + 1, d, core], ring_s.at[s, d], ring_r.at[s, d], (right, left)[d])

    def sib(s, d):
        return remote(x.at[s, d, core], x.at[s, d, core], sib_s.at[s, d], sib_r.at[s, d], sibling)

    def lead_swap(g, t):
        at = lead_cols(t)
        return remote(pb.at[0, g, 1 - col, :, at], rv.at[0, g, :, at], lead_s.at[g, t], lead_r.at[g, t], across)

    def lead_sent(g):
        @pl.loop(0, leads)
        def _(t):
            lead_swap(g, t).wait_send()

    def swap(s, g):
        return remote(pb.at[s % keep, g, 1 - col], rv.at[s, g], y_s.at[s, g], y_r.at[s, g], across)

    def slot(s):
        return jnp.where(s == n - 1, 1, jnp.maximum(s - 1, 0))

    def share(s):
        return remote(rv.at[slot(s), col], rv.at[slot(s), col], y_s.at[s, 2], y_r.at[s, 2], across)

    def part_cols(k):
        return pl.ds(pl.multiple_of(k * piece, piece), piece)

    def down_sib(s, k):
        return remote(pd.at[s % 2, k, :, 1 - core], x.at[s, :, 1, :, part_cols(k)], ds_s.at[s, k], ds_r.at[s, k], sibling)

    def down_ring(s, d, k):
        return remote(pd.at[s % 2, k, d, core], x.at[(s + 1) % n, d, 0, :, part_cols(k)],
                      rs_s.at[s, d, k], rs_r.at[s, d, k], (right, left)[d])

    def product(s, g, w):
        with jax.named_scope("product"):
            @pl.loop(0, units // tile)
            def _(t):
                at = pl.ds(pl.multiple_of(t * tile, tile), tile)
                part = jnp.dot(x[s].reshape(4 * half, width), w[:, at], preferred_element_type=F32)
                pb[s % keep, g, :, :, at] = part.astype(BF).reshape(2, 2 * half, tile)
            swap(s, g).start()

    def activate(s):
        with jax.named_scope("activate"):
            scale_sib(s).wait_recv()
            scale = sc[s].reshape(2 * half, 128)[:, 0:1]

            @pl.loop(0, leads)
            def _(t):
                at = lead_cols(t)
                gate = scale * (pb[s % keep, 0, col, :, at].astype(F32) + rv[s, 0, :, at].astype(F32))
                up = scale * (pb[s % keep, 1, col, :, at].astype(F32) + rv[s, 1, :, at].astype(F32))
                hidden = (gate / (1.0 + jnp.exp(-gate)) * up).astype(BF)
                if isinstance(s, int) and s == 0:
                    kept[:, at] = hidden
                else:
                    rv[slot(s), col, :, at] = hidden

    def finish(s):
        swap(s, 0).wait_recv()
        swap(s, 1).wait_recv()
        activate(s)
        share(s).start()

    def pass_on(s):
        with jax.named_scope("pass_on"):
            sib(s, 0).start()
            sib(s, 1).start()

            @pl.when(s < n - 1)
            def _():
                ring(s, 0).start()
                ring(s, 1).start()

    def retire(s):
        with jax.named_scope("retire"):
            for d in range(2):
                sib(s, d).wait_send()

            @pl.when(s < n - 1)
            def _():
                ring(s, 0).wait_send()
                ring(s, 1).wait_send()

            pl.semaphore_signal(free.at[s, 2], inc=1, device_id=sibling, device_id_type=MESH)

            @pl.when(s != 1)
            def _():
                pl.semaphore_signal(free.at[s, 0], inc=1, device_id=left, device_id_type=MESH)
                pl.semaphore_signal(free.at[s, 1], inc=1, device_id=right, device_id_type=MESH)

    def sent(s):
        with jax.named_scope("sent"):
            @pl.loop(0, parts)
            def _(k):
                down_sib(s, k).wait_send()
                down_ring(s, 0, k).wait_send()
                down_ring(s, 1, k).wait_send()

    def down_part(s, k):
        h = rv[slot(s)].reshape(4 * half, units)
        part = jnp.dot(h, wd[:, part_cols(k)], preferred_element_type=F32).astype(BF)
        pd[s % 2, k] = part.reshape(2, 2, half, piece)
        down_sib(s, k).start()

    def stage_part(s, k):
        down_sib(s, k).wait_recv()
        for d in range(2):
            mine = pd[s % 2, k, d, core].astype(F32) + x[s, d, 1, :, part_cols(k)].astype(F32)

            @pl.when(s == 1)
            def _():
                pd[s % 2, k, d, core] = mine.astype(BF)

            @pl.when(s > 1)
            def _():
                down_ring(s - 1, d, k).wait_recv()
                pd[s % 2, k, d, core] = (mine + x[s, d, 0, :, part_cols(k)].astype(F32)).astype(BF)

            down_ring(s, d, k).start()

    def final_part(k):
        down_sib(0, k).wait_recv()
        for d in range(2):
            down_ring(n - 1, d, k).wait_recv()
            here = (slice(d * half, (d + 1) * half), part_cols(k))
            mine = pd[0, k, d, core].astype(F32) + x[0, d, 1, :, here[1]].astype(F32)
            mine = mine + x[0, d, 0, :, here[1]].astype(F32)
            out[here] = (out[here].astype(F32) + mine).astype(BF)

    def ring_free(s):
        pl.semaphore_wait(free.at[(s + 1) % n, 0], 1)
        pl.semaphore_wait(free.at[(s + 1) % n, 1], 1)

    def down(s):
        pl.semaphore_wait(free.at[s, 2], 1)
        with jax.named_scope("down"):
            @pl.loop(0, parts)
            def _(k):
                down_part(s, k)

    def stage(s):
        ring_free(s)
        with jax.named_scope("stage"):
            @pl.loop(0, parts)
            def _(k):
                stage_part(s, k)

    def last(s, follow):
        with jax.named_scope("last"):
            pl.semaphore_wait(free.at[s, 2], 1)

            @pl.loop(0, parts + 2)
            def _(k):
                @pl.when(k < parts)
                def _():
                    down_part(s, k)

                @pl.when(k > 1)
                def _():
                    follow(k - 2)

    met = greet((right, left, sibling, across))
    load_tok.start()

    @pl.loop(0, leads)
    def _(t):
        load_g(t).start()

    with jax.named_scope("tok"):
        load_tok.wait()
    gains = gain[...].astype(F32)
    squares = jnp.zeros((2 * half, 128), F32)
    for b in range(width // 128):
        at = slice(b * 128, (b + 1) * 128)
        wide = out[:, at].astype(F32)
        squares += wide * wide
        scaled = (wide * gains[b : b + 1]).astype(BF)
        x[0, 0, core, :, at] = scaled[:half]
        x[0, 1, core, :, at] = scaled[half:]
    sums = jnp.broadcast_to(jnp.sum(squares, axis=1, keepdims=True), squares.shape)
    sq[0] = sums[:half]
    sq[1] = sums[half:]
    with jax.named_scope("met"):
        met()
    pass_on(0)
    trade = remote(sq.at[1 - col], sq_in, sq_sem.at[0], sq_sem.at[1], across)
    trade.start()
    with jax.named_scope("sib0"):
        sib(0, 0).wait_recv()
        sib(0, 1).wait_recv()

    def lead_product(g, w, load):
        @pl.loop(0, leads)
        def _(t):
            load(t).wait()
            at = lead_cols(t)
            part = jnp.dot(x[0].reshape(4 * half, width), w[:, at], preferred_element_type=F32)
            pb[0, g, :, :, at] = part.astype(BF).reshape(2, 2 * half, lead)
            lead_swap(g, t).start()

            if g == 0:
                load_u(t).start()

    with jax.named_scope("lead0"):
        lead_product(0, wg, load_g)
    load_d.start()
    trade.wait()
    total = sq[col] + sq_in[...]
    sc[0, core] = 1.0 / jnp.sqrt(total / (width * cols) + floor_term)
    scale_on(0)
    with jax.named_scope("lead1"):
        lead_product(1, wu, load_u)
    with jax.named_scope("ring0"):
        ring(0, 0).wait_recv()
        ring(0, 1).wait_recv()
    pass_on(1)
    scale_ring(0).wait_recv()
    scale_on(1)

    @pl.loop(1, n)
    def _(i):
        sib(i, 0).wait_recv()
        sib(i, 1).wait_recv()

        @pl.when(i == keep)
        def _():
            lead_sent(0)

        @pl.when(i > keep)
        def _():
            swap(i - keep, 0).wait_send()

        product(i, 0, wg)

        @pl.when(i == 1)
        def _():
            @pl.loop(0, leads)
            def _(t):
                lead_swap(0, t).wait_recv()
                lead_swap(1, t).wait_recv()

            activate(0)

        @pl.when((i > 1) & (i < n - 1))
        def _():
            finish(i - 1)

        @pl.when(i == keep)
        def _():
            lead_sent(1)

        @pl.when(i > keep)
        def _():
            swap(i - keep, 1).wait_send()

        product(i, 1, wu)

        @pl.when(i < n - 1)
        def _():
            ring(i, 0).wait_recv()
            ring(i, 1).wait_recv()
            pass_on(i + 1)
            scale_ring(i).wait_recv()
            scale_on(i + 1)

        retire(i - 1)

        @pl.when(i > 3)
        def _():
            stage(i - 3)

        @pl.when(i == n - 1)
        def _():
            finish(i - 1)

        @pl.when(i == 3)
        def _():
            load_d.wait()

        @pl.when(i > 2)
        def _():
            share(i - 2).wait_recv()

            @pl.when(i > 4)
            def _():
                sent(i - 4)

            down(i - 2)

    retire(n - 1)
    stage(n - 3)
    share(1).wait_send()
    share(2).wait_send()
    rv[0, col] = kept[...]
    finish(n - 1)
    share(0).start()
    sent(n - 4)
    ring_free(n - 2)
    with jax.named_scope("share6"):
        share(n - 2).wait_recv()
    last(n - 2, lambda k: stage_part(n - 2, k))
    sent(n - 3)
    ring_free(n - 1)
    with jax.named_scope("share7"):
        share(n - 1).wait_recv()
    last(n - 1, lambda k: stage_part(n - 1, k))
    sent(n - 2)
    with jax.named_scope("share0"):
        share(0).wait_recv()
    last(0, final_part)

    sent(n - 1)

    @pl.loop(0, parts)
    def _(k):
        down_sib(0, k).wait_send()

    @pl.loop(n - keep, n)
    def _(s):
        swap(s, 0).wait_send()
        swap(s, 1).wait_send()

    @pl.loop(0, n)
    def _(s):
        @pl.when((s < 1) | (s > 2))
        def _():
            share(s).wait_send()

        scale_sib(s).wait_send()

        @pl.when(s < n - 1)
        def _():
            scale_ring(s).wait_send()


def kernels(rows, cols, tokens, norm_gain, gate_proj, up_proj, down_proj):
    n = rows // 2
    count, width = tokens.shape
    half = count // 2
    units = gate_proj.shape[1]
    lead = 256 if units % 256 == 0 else 128
    tile = units // 2 if units % 256 == 0 else lead
    parts = 4
    piece = width // parts
    vmem, hbm = pl.BlockSpec(memory_space=pltpu.VMEM), pl.BlockSpec(memory_space=pl.ANY)
    dma = pltpu.SemaphoreType.DMA
    return pl.pallas_call(
        functools.partial(fused_kernel, rows, cols, tile, lead),
        out_shape=jax.ShapeDtypeStruct(tokens.shape, BF),
        in_specs=[hbm, vmem, hbm, hbm, hbm],
        out_specs=vmem,
        scratch_shapes=[
            pltpu.VMEM(gate_proj.shape, BF),
            pltpu.VMEM(up_proj.shape, BF),
            pltpu.VMEM(down_proj.shape, BF),
            pltpu.VMEM((n, 2, 2, half, width), BF),
            pltpu.VMEM((4, 2, 2, 2 * half, units), BF),
            pltpu.VMEM((n, 2, 2 * half, units), BF),
            pltpu.VMEM((2, parts, 2, 2, half, piece), BF),
            pltpu.VMEM((2 * half, units), BF),
            pltpu.VMEM((2, half, 128), F32),
            pltpu.VMEM((half, 128), F32),
            pltpu.VMEM((n, 2, half, 128), F32),
            dma, dma((units // lead,)), dma((units // lead,)), dma, dma((2,)),
            dma((n, 2)), dma((n, 2)), dma((n, 2)), dma((n, 2)),
            dma((2, units // lead)), dma((2, units // lead)),
            dma((n, 3)), dma((n, 3)),
            dma((n, parts)), dma((n, parts)), dma((n, 2, parts)), dma((n, 2, parts)),
            dma((n, 2)), dma((n, 2)),
            pltpu.SemaphoreType.REGULAR((n, 3)),
        ],
        compiler_params=pltpu.CompilerParams(
            collective_id=0, has_side_effects=True, vmem_limit_bytes=67043328
        ),
    )(tokens, norm_gain.reshape(width // 128, 128), gate_proj, up_proj, down_proj)


def plain(rows, cols, tokens, norm_gain, gate_proj, up_proj, down_proj):
    gathered = lax.all_gather(tokens, "row", axis=0, tiled=True)
    widened = gathered.astype(jnp.float32)
    partial_squares = jnp.sum(widened * widened, axis=1)
    scaled = (widened * norm_gain.astype(jnp.float32)[None, :]).astype(jnp.bfloat16)
    gate_part = jnp.dot(scaled, gate_proj, preferred_element_type=jnp.float32)
    up_part = jnp.dot(scaled, up_proj, preferred_element_type=jnp.float32)
    gate_sum, up_sum, block_squares = (
        lax.psum_scatter(
            gate_part.astype(jnp.bfloat16), "col", scatter_dimension=0, tiled=True
        ).astype(jnp.float32),
        lax.psum_scatter(
            up_part.astype(jnp.bfloat16), "col", scatter_dimension=0, tiled=True
        ).astype(jnp.float32),
        lax.psum_scatter(
            partial_squares.astype(jnp.bfloat16), "col", scatter_dimension=0, tiled=True
        ).astype(jnp.float32),
    )
    row_scale = 1.0 / jnp.sqrt(block_squares / (tokens.shape[1] * cols) + floor_term)
    gate_value = row_scale[:, None] * gate_sum
    up_value = row_scale[:, None] * up_sum
    hidden = (jax.nn.silu(gate_value) * up_value).astype(jnp.bfloat16)
    partial_out = jnp.dot(
        lax.all_gather(hidden, "col", axis=0, tiled=True),
        down_proj,
        preferred_element_type=jnp.float32,
    )
    summed = lax.psum_scatter(
        partial_out.astype(jnp.bfloat16), "row", scatter_dimension=0, tiled=True
    ).astype(jnp.float32)
    return (tokens.astype(jnp.float32) + summed).astype(jnp.bfloat16)


def solution(mesh):
    rows, cols = mesh.shape["row"], mesh.shape["col"]
    body = kernels if cols == 2 and rows % 4 == 0 and rows >= 16 else plain
    in_specs = (P("row", "col"), P("col"), P("col", "row"), P("col", "row"), P("row", "col"))
    out_specs = P("row", "col")
    return jax.shard_map(
        functools.partial(body, rows, cols), mesh=mesh, in_specs=in_specs, out_specs=out_specs, check_vma=False
    )
```

```python
import functools

import jax
import jax.numpy as jnp
from jax import lax
from jax.experimental import pallas as pl
from jax.experimental.pallas import tpu as pltpu
from jax.sharding import PartitionSpec as P

floor_term = 0.25
MESH = pl.DeviceIdType.MESH
BF = jnp.bfloat16
F32 = jnp.float32


def places(rows):
    n = rows // 2
    row, col = lax.axis_index("row"), lax.axis_index("col")
    core, chip = row % 2, row // 2
    z, x = chip // 2, chip % 2
    pos = z + x * (n - 1 - 2 * z)

    def at(p):
        p = (p + n) % n
        far = (2 * p) // n
        return ((1 - far) * 2 * p + far * (2 * (n - 1 - p) + 1)) * 2 + core

    right, left = (at(pos + 1), col), (at(pos - 1), col)
    return core, col, right, left, (row + 1 - 2 * core, col), (row, 1 - col)


def greet(partners):
    barrier = pltpu.get_barrier_semaphore()
    for device in partners:
        pl.semaphore_signal(barrier, inc=1, device_id=device, device_id_type=MESH)
    return lambda: pl.semaphore_wait(barrier, len(partners))


def remote(src, dst, send, recv, device):
    return pltpu.make_async_remote_copy(
        src_ref=src, dst_ref=dst, send_sem=send, recv_sem=recv, device_id=device, device_id_type=MESH
    )


def fused_kernel(rows, cols, tile, lead, tok_hbm, gain, wg_hbm, wu_hbm, wd_hbm, out, wg, wu, wd, x, pb, rv, pd, kept, sq, sq_in, sc,
                 tok_sem, w_sem, wd_sem, sq_sem, ring_s, ring_r, sib_s, sib_r, y_s, y_r,
                 ds_s, ds_r, rs_s, rs_r, sc_s, sc_r, free):
    n = rows // 2
    half, width = out.shape[0] // 2, out.shape[1]
    units = wg.shape[1]
    leads = units // lead
    keep = pb.shape[0]
    parts, piece = pd.shape[1], pd.shape[5]
    core, col, right, left, sibling, across = places(rows)
    load_tok = pltpu.make_async_copy(tok_hbm, out, tok_sem)
    load_d = pltpu.make_async_copy(wd_hbm, wd, wd_sem)

    def lead_cols(t):
        return pl.ds(pl.multiple_of(t * lead, lead), lead)

    def load_g(t):
        return pltpu.make_async_copy(wg_hbm.at[:, lead_cols(t)], wg.at[:, lead_cols(t)], w_sem.at[t])

    def load_u(t):
        return pltpu.make_async_copy(wu_hbm.at[:, lead_cols(t)], wu.at[:, lead_cols(t)], w_sem.at[t])

    def scale_ring(s):
        onward = (jnp.where(col == 0, right[0], left[0]), col)
        return remote(sc.at[s, core], sc.at[s + 1, core], sc_s.at[s % 2, 0], sc_r.at[s, 0], onward)

    def scale_sib(s):
        return remote(sc.at[s, core], sc.at[s, core], sc_s.at[s % 2, 1], sc_r.at[s, 1], sibling)

    def scale_on(s):
        @pl.when(s > 1)
        def _():
            scale_sib(s - 2).wait_send()
            scale_ring(s - 2).wait_send()

        scale_sib(s).start()

        @pl.when(s < n - 1)
        def _():
            scale_ring(s).start()

    def ring(s, d):
        return remote(x.at[s, d, core], x.at[s + 1, d, core], ring_s.at[s % 2, d], ring_r.at[s, d], (right, left)[d])

    def sib(s):
        return remote(x.at[s, :, core], x.at[s, :, core], sib_s.at[s % 2], sib_r.at[s], sibling)

    def swap(s, g, at=slice(None)):
        return remote(pb.at[s % keep, g, 1 - col, :, at], rv.at[s, g, :, at], y_s.at[s % keep, g], y_r.at[s % keep, g], across)

    def slot(s):
        return jnp.where(s == n - 1, 1, jnp.maximum(s - 1, 0))

    def share(s):
        return remote(rv.at[slot(s), col], rv.at[slot(s), col], y_s.at[s % keep, 2], y_r.at[s % keep, 2], across)

    def part_cols(k):
        return pl.ds(pl.multiple_of(k * piece, piece), piece)

    def down_sib(s, k):
        return remote(pd.at[s % 2, k, :, 1 - core], x.at[s, :, 1, :, part_cols(k)], ds_s.at[s % 2, k], ds_r.at[jnp.where(s == 0, 2, s % 2), k], sibling)

    def down_ring(s, d, k):
        return remote(pd.at[s % 2, k, d, core], x.at[(s + 1) % n, d, 0, :, part_cols(k)],
                      rs_s.at[s % 2, d, k], rs_r.at[jnp.where(s == n - 1, 2, s % 2), d, k], (right, left)[d])

    def product(s, g, w):
        with jax.named_scope("product"):
            @pl.loop(0, units // tile)
            def _(t):
                at = pl.ds(pl.multiple_of(t * tile, tile), tile)
                part = jnp.dot(x[s].reshape(4 * half, width), w[:, at], preferred_element_type=F32)
                pb[s % keep, g, :, :, at] = part.astype(BF).reshape(2, 2 * half, tile)
                swap(s, g, at).start()

    def activate(s):
        with jax.named_scope("activate"):
            scale_sib(s).wait_recv()
            scale = sc[s].reshape(2 * half, 128)[:, 0:1]

            @pl.loop(0, leads)
            def _(t):
                at = lead_cols(t)
                gate = scale * (pb[s % keep, 0, col, :, at].astype(F32) + rv[s, 0, :, at].astype(F32))
                up = scale * (pb[s % keep, 1, col, :, at].astype(F32) + rv[s, 1, :, at].astype(F32))
                hidden = (gate / (1.0 + jnp.exp(-gate)) * up).astype(BF)
                if isinstance(s, int) and s == 0:
                    kept[:, at] = hidden
                else:
                    rv[slot(s), col, :, at] = hidden

    def finish(s):
        swap(s, 0).wait_recv()
        swap(s, 1).wait_recv()
        activate(s)

        @pl.when(s > keep)
        def _():
            share(s - keep).wait_send()

        share(s).start()

    def pass_on(s):
        with jax.named_scope("pass_on"):
            sib(s).start()

            @pl.when(s < n - 1)
            def _():
                ring(s, 0).start()
                ring(s, 1).start()

    def retire(s):
        with jax.named_scope("retire"):
            sib(s).wait_send()

            @pl.when(s < n - 1)
            def _():
                ring(s, 0).wait_send()
                ring(s, 1).wait_send()

            pl.semaphore_signal(free.at[s, 2], inc=1, device_id=sibling, device_id_type=MESH)

            @pl.when(s != 1)
            def _():
                pl.semaphore_signal(free.at[s, 0], inc=1, device_id=left, device_id_type=MESH)
                pl.semaphore_signal(free.at[s, 1], inc=1, device_id=right, device_id_type=MESH)

    def sent(s):
        with jax.named_scope("sent"):
            @pl.loop(0, parts)
            def _(k):
                down_sib(s, k).wait_send()
                down_ring(s, 0, k).wait_send()
                down_ring(s, 1, k).wait_send()

    def down_part(s, k):
        h = rv[slot(s)].reshape(4 * half, units)
        part = jnp.dot(h, wd[:, part_cols(k)], preferred_element_type=F32).astype(BF)
        pd[s % 2, k] = part.reshape(2, 2, half, piece)
        down_sib(s, k).start()

    def stage_part(s, k):
        down_sib(s, k).wait_recv()
        for d in range(2):
            mine = pd[s % 2, k, d, core].astype(F32) + x[s, d, 1, :, part_cols(k)].astype(F32)

            @pl.when(s == 1)
            def _():
                pd[s % 2, k, d, core] = mine.astype(BF)

            @pl.when(s > 1)
            def _():
                down_ring(s - 1, d, k).wait_recv()
                pd[s % 2, k, d, core] = (mine + x[s, d, 0, :, part_cols(k)].astype(F32)).astype(BF)

            down_ring(s, d, k).start()

    def final_part(k):
        down_sib(0, k).wait_recv()
        for d in range(2):
            down_ring(n - 1, d, k).wait_recv()
            here = (slice(d * half, (d + 1) * half), part_cols(k))
            mine = pd[0, k, d, core].astype(F32) + x[0, d, 1, :, here[1]].astype(F32)
            mine = mine + x[0, d, 0, :, here[1]].astype(F32)
            out[here] = (out[here].astype(F32) + mine).astype(BF)

    def ring_free(s):
        pl.semaphore_wait(free.at[(s + 1) % n, 0], 1)
        pl.semaphore_wait(free.at[(s + 1) % n, 1], 1)

    def down(s):
        pl.semaphore_wait(free.at[s, 2], 1)
        with jax.named_scope("down"):
            @pl.loop(0, parts)
            def _(k):
                down_part(s, k)

    def stage(s):
        ring_free(s)
        with jax.named_scope("stage"):
            @pl.loop(0, parts)
            def _(k):
                stage_part(s, k)

    def last(s, follow):
        with jax.named_scope("last"):
            pl.semaphore_wait(free.at[s, 2], 1)

            @pl.loop(0, parts + 2)
            def _(k):
                @pl.when(k < parts)
                def _():
                    down_part(s, k)

                @pl.when(k > 1)
                def _():
                    follow(k - 2)

    met = greet((right, left, sibling, across))
    load_tok.start()

    @pl.loop(0, leads)
    def _(t):
        load_g(t).start()

    with jax.named_scope("tok"):
        load_tok.wait()
    gains = gain[...].astype(F32)
    squares = jnp.zeros((2 * half, 128), F32)
    for b in range(width // 128):
        at = slice(b * 128, (b + 1) * 128)
        wide = out[:, at].astype(F32)
        squares += wide * wide
        scaled = (wide * gains[b : b + 1]).astype(BF)
        x[0, 0, core, :, at] = scaled[:half]
        x[0, 1, core, :, at] = scaled[half:]
    sums = jnp.broadcast_to(jnp.sum(squares, axis=1, keepdims=True), squares.shape)
    sq[0] = sums[:half]
    sq[1] = sums[half:]
    with jax.named_scope("met"):
        met()
    pass_on(0)
    trade = remote(sq.at[1 - col], sq_in, sq_sem.at[0], sq_sem.at[1], across)
    trade.start()
    with jax.named_scope("sib0"):
        sib(0).wait_recv()

    def lead_product(g, w, load):
        @pl.loop(0, leads)
        def _(t):
            load(t).wait()
            at = lead_cols(t)
            part = jnp.dot(x[0].reshape(4 * half, width), w[:, at], preferred_element_type=F32)
            pb[0, g, :, :, at] = part.astype(BF).reshape(2, 2 * half, lead)
            swap(0, g, at).start()

            if g == 0:
                load_u(t).start()
            else:

                @pl.when(t == leads - 2)
                def _():
                    ring(0, 0).wait_recv()
                    ring(0, 1).wait_recv()
                    pass_on(1)
                    scale_ring(0).wait_recv()
                    scale_on(1)

    with jax.named_scope("lead0"):
        lead_product(0, wg, load_g)
    load_d.start()
    trade.wait()
    total = sq[col] + sq_in[...]
    sc[0, core] = 1.0 / jnp.sqrt(total / (width * cols) + floor_term)
    scale_on(0)
    with jax.named_scope("lead1"):
        lead_product(1, wu, load_u)

    @pl.loop(1, n)
    def _(i):
        sib(i).wait_recv()

        @pl.when(i >= keep)
        def _():
            swap(i - keep, 0).wait_send()

        product(i, 0, wg)

        @pl.when(i == 1)
        def _():
            swap(0, 0).wait_recv()
            swap(0, 1).wait_recv()
            activate(0)

        @pl.when((i > 1) & (i < n - 1))
        def _():
            finish(i - 1)

        @pl.when(i >= keep)
        def _():
            swap(i - keep, 1).wait_send()

        product(i, 1, wu)

        @pl.when(i > 3)
        def _():
            stage(i - 3)

        retire(i - 1)

        @pl.when(i < n - 1)
        def _():
            ring(i, 0).wait_recv()
            ring(i, 1).wait_recv()
            pass_on(i + 1)
            scale_ring(i).wait_recv()
            scale_on(i + 1)

        @pl.when(i == n - 1)
        def _():
            finish(i - 1)

        @pl.when(i == 3)
        def _():
            load_d.wait()

        @pl.when(i > 2)
        def _():
            share(i - 2).wait_recv()

            @pl.when(i > 4)
            def _():
                sent(i - 4)

            down(i - 2)

    stage(n - 3)
    retire(n - 1)
    rv[0, col] = kept[...]
    finish(n - 1)
    again = (n - 1) // keep * keep
    share(again).wait_send()
    share(0).start()
    sent(n - 4)
    ring_free(n - 2)
    with jax.named_scope("share6"):
        share(n - 2).wait_recv()
    last(n - 2, lambda k: stage_part(n - 2, k))
    sent(n - 3)
    ring_free(n - 1)
    with jax.named_scope("share7"):
        share(n - 1).wait_recv()
    last(n - 1, lambda k: stage_part(n - 1, k))
    sent(n - 2)
    with jax.named_scope("share0"):
        share(0).wait_recv()
    last(0, final_part)

    sent(n - 1)

    @pl.loop(0, parts)
    def _(k):
        down_sib(0, k).wait_send()

    @pl.loop(n - keep, n)
    def _(s):
        swap(s, 0).wait_send()
        swap(s, 1).wait_send()

    for s in [0] + [s for s in range(n - keep, n) if s != again]:
        share(s).wait_send()
    scale_sib(n - 2).wait_send()
    scale_ring(n - 2).wait_send()
    scale_sib(n - 1).wait_send()


def kernels(rows, cols, tokens, norm_gain, gate_proj, up_proj, down_proj):
    n = rows // 2
    count, width = tokens.shape
    half = count // 2
    units = gate_proj.shape[1]
    lead = 256 if units % 256 == 0 else 128
    tile = units // 2 if units % 256 == 0 else lead
    parts = 4
    piece = width // parts
    vmem, hbm = pl.BlockSpec(memory_space=pltpu.VMEM), pl.BlockSpec(memory_space=pl.ANY)
    dma = pltpu.SemaphoreType.DMA
    return pl.pallas_call(
        functools.partial(fused_kernel, rows, cols, tile, lead),
        out_shape=jax.ShapeDtypeStruct(tokens.shape, BF),
        in_specs=[hbm, vmem, hbm, hbm, hbm],
        out_specs=vmem,
        scratch_shapes=[
            pltpu.VMEM(gate_proj.shape, BF),
            pltpu.VMEM(up_proj.shape, BF),
            pltpu.VMEM(down_proj.shape, BF),
            pltpu.VMEM((n, 2, 2, half, width), BF),
            pltpu.VMEM((4, 2, 2, 2 * half, units), BF),
            pltpu.VMEM((n, 2, 2 * half, units), BF),
            pltpu.VMEM((2, parts, 2, 2, half, piece), BF),
            pltpu.VMEM((2 * half, units), BF),
            pltpu.VMEM((2, half, 128), F32),
            pltpu.VMEM((half, 128), F32),
            pltpu.VMEM((n, 2, half, 128), F32),
            dma, dma((units // lead,)), dma, dma((2,)),
            dma((2, 2)), dma((n, 2)), dma((2,)), dma((n,)), dma((4, 3)), dma((4, 3)),
            dma((2, parts)), dma((3, parts)), dma((2, 2, parts)), dma((3, 2, parts)),
            dma((2, 2)), dma((n, 2)),
            pltpu.SemaphoreType.REGULAR((n, 3)),
        ],
        compiler_params=pltpu.CompilerParams(
            collective_id=0, has_side_effects=True, vmem_limit_bytes=67043328
        ),
    )(tokens, norm_gain.reshape(width // 128, 128), gate_proj, up_proj, down_proj)


def plain(rows, cols, tokens, norm_gain, gate_proj, up_proj, down_proj):
    gathered = lax.all_gather(tokens, "row", axis=0, tiled=True)
    widened = gathered.astype(jnp.float32)
    partial_squares = jnp.sum(widened * widened, axis=1)
    scaled = (widened * norm_gain.astype(jnp.float32)[None, :]).astype(jnp.bfloat16)
    gate_part = jnp.dot(scaled, gate_proj, preferred_element_type=jnp.float32)
    up_part = jnp.dot(scaled, up_proj, preferred_element_type=jnp.float32)
    gate_sum, up_sum, block_squares = (
        lax.psum_scatter(
            gate_part.astype(jnp.bfloat16), "col", scatter_dimension=0, tiled=True
        ).astype(jnp.float32),
        lax.psum_scatter(
            up_part.astype(jnp.bfloat16), "col", scatter_dimension=0, tiled=True
        ).astype(jnp.float32),
        lax.psum_scatter(
            partial_squares.astype(jnp.bfloat16), "col", scatter_dimension=0, tiled=True
        ).astype(jnp.float32),
    )
    row_scale = 1.0 / jnp.sqrt(block_squares / (tokens.shape[1] * cols) + floor_term)
    gate_value = row_scale[:, None] * gate_sum
    up_value = row_scale[:, None] * up_sum
    hidden = (jax.nn.silu(gate_value) * up_value).astype(jnp.bfloat16)
    partial_out = jnp.dot(
        lax.all_gather(hidden, "col", axis=0, tiled=True),
        down_proj,
        preferred_element_type=jnp.float32,
    )
    summed = lax.psum_scatter(
        partial_out.astype(jnp.bfloat16), "row", scatter_dimension=0, tiled=True
    ).astype(jnp.float32)
    return (tokens.astype(jnp.float32) + summed).astype(jnp.bfloat16)


def solution(mesh):
    rows, cols = mesh.shape["row"], mesh.shape["col"]
    body = kernels if cols == 2 and rows % 4 == 0 and rows >= 16 else plain
    in_specs = (P("row", "col"), P("col"), P("col", "row"), P("col", "row"), P("row", "col"))
    out_specs = P("row", "col")
    return jax.shard_map(
        functools.partial(body, rows, cols), mesh=mesh, in_specs=in_specs, out_specs=out_specs, check_vma=False
    )
```

```python
import functools

import jax
import jax.numpy as jnp
from jax import lax
from jax.experimental import pallas as pl
from jax.experimental.pallas import tpu as pltpu
from jax.sharding import PartitionSpec as P

floor_term = 0.25
MESH = pl.DeviceIdType.MESH
BF = jnp.bfloat16
F32 = jnp.float32


def places(rows):
    n = rows // 2
    row, col = lax.axis_index("row"), lax.axis_index("col")
    core, chip = row % 2, row // 2
    z, x = chip // 2, chip % 2
    pos = z + x * (n - 1 - 2 * z)

    def at(p):
        p = (p + n) % n
        far = (2 * p) // n
        return ((1 - far) * 2 * p + far * (2 * (n - 1 - p) + 1)) * 2 + core

    right, left = (at(pos + 1), col), (at(pos - 1), col)
    return core, col, right, left, (row + 1 - 2 * core, col), (row, 1 - col)


def greet(partners):
    barrier = pltpu.get_barrier_semaphore()
    for device in partners:
        pl.semaphore_signal(barrier, inc=1, device_id=device, device_id_type=MESH)
    return lambda: pl.semaphore_wait(barrier, len(partners))


def remote(src, dst, send, recv, device):
    return pltpu.make_async_remote_copy(
        src_ref=src, dst_ref=dst, send_sem=send, recv_sem=recv, device_id=device, device_id_type=MESH
    )


def fused_kernel(rows, cols, tile, lead, tok_hbm, gain, wg_hbm, wu_hbm, wd_hbm, out, wg, wu, wd, x, pb, rv, pd, kept, sq, sq_in, sc,
                 tok_sem, w_sem, wd_sem, sq_sem, ring_s, ring_r, sib_s, sib_r, y_s, y_r,
                 ds_s, ds_r, rs_s, rs_r, sc_s, sc_r, free):
    n = rows // 2
    half, width = out.shape[0] // 2, out.shape[1]
    units = wg.shape[1]
    leads = units // lead
    keep = pb.shape[0]
    parts, piece = pd.shape[1], pd.shape[5]
    core, col, right, left, sibling, across = places(rows)
    load_tok = pltpu.make_async_copy(tok_hbm, out, tok_sem)
    load_d = pltpu.make_async_copy(wd_hbm, wd, wd_sem)

    def lead_cols(t):
        return pl.ds(pl.multiple_of(t * lead, lead), lead)

    def load_g(t):
        return pltpu.make_async_copy(wg_hbm.at[:, lead_cols(t)], wg.at[:, lead_cols(t)], w_sem.at[t])

    def load_u(t):
        return pltpu.make_async_copy(wu_hbm.at[:, lead_cols(t)], wu.at[:, lead_cols(t)], w_sem.at[t])

    def scale_ring(s):
        onward = (jnp.where(col == 0, right[0], left[0]), col)
        return remote(sc.at[s, core], sc.at[s + 1, core], sc_s.at[s % 2, 0], sc_r.at[s, 0], onward)

    def scale_sib(s):
        return remote(sc.at[s, core], sc.at[s, core], sc_s.at[s % 2, 1], sc_r.at[s, 1], sibling)

    def scale_on(s):
        @pl.when(s > 1)
        def _():
            scale_sib(s - 2).wait_send()
            scale_ring(s - 2).wait_send()

        scale_sib(s).start()

        @pl.when(s < n - 1)
        def _():
            scale_ring(s).start()

    def ring(s, d):
        return remote(x.at[s, d, core], x.at[s + 1, d, core], ring_s.at[s % 2, d], ring_r.at[s, d], (right, left)[d])

    def sib(s):
        return remote(x.at[s, :, core], x.at[s, :, core], sib_s.at[s % 2], sib_r.at[s], sibling)

    def swap(s, g, at=slice(None)):
        return remote(pb.at[s % keep, g, 1 - col, :, at], rv.at[s, g, :, at], y_s.at[s % keep, g], y_r.at[s % keep, g], across)

    def slot(s):
        return jnp.where(s == n - 1, 1, jnp.maximum(s - 1, 0))

    def share(s):
        return remote(rv.at[slot(s), col], rv.at[slot(s), col], y_s.at[s % keep, 2], y_r.at[s % keep, 2], across)

    def part_cols(k):
        return pl.ds(pl.multiple_of(k * piece, piece), piece)

    def down_sib(s, k):
        return remote(pd.at[s % 2, k, :, 1 - core], x.at[s, :, 1, :, part_cols(k)], ds_s.at[s % 2, k], ds_r.at[jnp.where(s == 0, 2, s % 2), k], sibling)

    def down_ring(s, d, k):
        return remote(pd.at[s % 2, k, d, core], x.at[(s + 1) % n, d, 0, :, part_cols(k)],
                      rs_s.at[s % 2, d, k], rs_r.at[jnp.where(s == n - 1, 2, s % 2), d, k], (right, left)[d])

    def product(s, g, w):
        with jax.named_scope("product"):
            @pl.loop(0, units // tile)
            def _(t):
                at = pl.ds(pl.multiple_of(t * tile, tile), tile)
                part = jnp.dot(x[s].reshape(4 * half, width), w[:, at], preferred_element_type=F32)
                pb[s % keep, g, :, :, at] = part.astype(BF).reshape(2, 2 * half, tile)
                swap(s, g, at).start()

    def activate(s):
        with jax.named_scope("activate"):
            scale_sib(s).wait_recv()
            scale = sc[s].reshape(2 * half, 128)[:, 0:1]

            @pl.loop(0, leads)
            def _(t):
                at = lead_cols(t)
                gate = scale * (pb[s % keep, 0, col, :, at].astype(F32) + rv[s, 0, :, at].astype(F32))
                up = scale * (pb[s % keep, 1, col, :, at].astype(F32) + rv[s, 1, :, at].astype(F32))
                hidden = (gate / (1.0 + jnp.exp(-gate)) * up).astype(BF)
                if isinstance(s, int) and s == 0:
                    kept[:, at] = hidden
                else:
                    rv[slot(s), col, :, at] = hidden

    def finish(s):
        swap(s, 0).wait_recv()
        swap(s, 1).wait_recv()
        activate(s)

        @pl.when(s > keep)
        def _():
            share(s - keep).wait_send()

        share(s).start()

    def pass_on(s):
        with jax.named_scope("pass_on"):
            sib(s).start()

            @pl.when(s < n - 1)
            def _():
                ring(s, 0).start()
                ring(s, 1).start()

    def retire(s):
        with jax.named_scope("retire"):
            sib(s).wait_send()

            @pl.when(s < n - 1)
            def _():
                ring(s, 0).wait_send()
                ring(s, 1).wait_send()

            pl.semaphore_signal(free.at[s, 2], inc=1, device_id=sibling, device_id_type=MESH)

            @pl.when(s != 1)
            def _():
                pl.semaphore_signal(free.at[s, 0], inc=1, device_id=left, device_id_type=MESH)
                pl.semaphore_signal(free.at[s, 1], inc=1, device_id=right, device_id_type=MESH)

    def sent(s):
        with jax.named_scope("sent"):
            @pl.loop(0, parts)
            def _(k):
                down_sib(s, k).wait_send()
                down_ring(s, 0, k).wait_send()
                down_ring(s, 1, k).wait_send()

    def down_part(s, k):
        h = rv[slot(s)].reshape(4 * half, units)
        part = jnp.dot(h, wd[:, part_cols(k)], preferred_element_type=F32).astype(BF)
        pd[s % 2, k] = part.reshape(2, 2, half, piece)
        down_sib(s, k).start()

    def stage_part(s, k):
        down_sib(s, k).wait_recv()
        for d in range(2):
            mine = pd[s % 2, k, d, core].astype(F32) + x[s, d, 1, :, part_cols(k)].astype(F32)

            @pl.when(s == 1)
            def _():
                pd[s % 2, k, d, core] = mine.astype(BF)

            @pl.when(s > 1)
            def _():
                down_ring(s - 1, d, k).wait_recv()
                pd[s % 2, k, d, core] = (mine + x[s, d, 0, :, part_cols(k)].astype(F32)).astype(BF)

            down_ring(s, d, k).start()

    def final_part(k):
        down_sib(0, k).wait_recv()
        for d in range(2):
            down_ring(n - 1, d, k).wait_recv()
            here = (slice(d * half, (d + 1) * half), part_cols(k))
            mine = pd[0, k, d, core].astype(F32) + x[0, d, 1, :, here[1]].astype(F32)
            mine = mine + x[0, d, 0, :, here[1]].astype(F32)
            out[here] = (out[here].astype(F32) + mine).astype(BF)

    def ring_free(s):
        pl.semaphore_wait(free.at[(s + 1) % n, 0], 1)
        pl.semaphore_wait(free.at[(s + 1) % n, 1], 1)

    def down(s):
        pl.semaphore_wait(free.at[s, 2], 1)
        with jax.named_scope("down"):
            @pl.loop(0, parts)
            def _(k):
                down_part(s, k)

    def stage(s):
        ring_free(s)
        with jax.named_scope("stage"):
            @pl.loop(0, parts)
            def _(k):
                stage_part(s, k)

    def last(s, follow):
        with jax.named_scope("last"):
            pl.semaphore_wait(free.at[s, 2], 1)

            @pl.loop(0, parts + 2)
            def _(k):
                @pl.when(k < parts)
                def _():
                    down_part(s, k)

                @pl.when(k > 1)
                def _():
                    follow(k - 2)

    met = greet((right, left, sibling, across))
    load_tok.start()

    @pl.loop(0, leads)
    def _(t):
        load_g(t).start()

    with jax.named_scope("tok"):
        load_tok.wait()
    gains = gain[...].astype(F32)
    squares = jnp.zeros((2 * half, 128), F32)
    for b in range(width // 128):
        at = slice(b * 128, (b + 1) * 128)
        wide = out[:, at].astype(F32)
        squares += wide * wide
        scaled = (wide * gains[b : b + 1]).astype(BF)
        x[0, 0, core, :, at] = scaled[:half]
        x[0, 1, core, :, at] = scaled[half:]
    sums = jnp.broadcast_to(jnp.sum(squares, axis=1, keepdims=True), squares.shape)
    sq[0] = sums[:half]
    sq[1] = sums[half:]
    with jax.named_scope("met"):
        met()
    pass_on(0)
    trade = remote(sq.at[1 - col], sq_in, sq_sem.at[0], sq_sem.at[1], across)
    trade.start()
    early = min(3, leads - 2)

    def lead_rows(t, c):
        at, rows_at = lead_cols(t), pl.ds(pl.multiple_of(c * half, half), half)
        part = jnp.dot(x[0, :, c].reshape(2 * half, width), wg[:, at], preferred_element_type=F32)
        pb[0, 0, :, rows_at, at] = part.astype(BF).reshape(2, half, lead)
        remote(pb.at[0, 0, 1 - col, rows_at, at], rv.at[0, 0, rows_at, at], y_s.at[0, 0], y_r.at[0, 0], across).start()

    @pl.loop(0, early)
    def _(t):
        load_g(t).wait()
        lead_rows(t, core)

    sib(0).wait_recv()

    @pl.loop(0, early)
    def _(t):
        lead_rows(t, 1 - core)
        load_u(t).start()

    def lead_product(g, w, load):
        @pl.loop(0 if g else early, leads)
        def _(t):
            load(t).wait()
            at = lead_cols(t)
            part = jnp.dot(x[0].reshape(4 * half, width), w[:, at], preferred_element_type=F32)
            pb[0, g, :, :, at] = part.astype(BF).reshape(2, 2 * half, lead)
            swap(0, g, at).start()

            if g == 0:
                load_u(t).start()
            else:

                @pl.when(t == leads - 2)
                def _():
                    ring(0, 0).wait_recv()
                    ring(0, 1).wait_recv()
                    pass_on(1)
                    scale_ring(0).wait_recv()
                    scale_on(1)

    with jax.named_scope("lead0"):
        lead_product(0, wg, load_g)
    load_d.start()
    trade.wait()
    total = sq[col] + sq_in[...]
    sc[0, core] = 1.0 / jnp.sqrt(total / (width * cols) + floor_term)
    scale_on(0)
    with jax.named_scope("lead1"):
        lead_product(1, wu, load_u)

    @pl.loop(1, n)
    def _(i):
        sib(i).wait_recv()

        @pl.when(i >= keep)
        def _():
            swap(i - keep, 0).wait_send()

        product(i, 0, wg)

        @pl.when(i == 1)
        def _():
            swap(0, 0).wait_recv()
            swap(0, 1).wait_recv()
            activate(0)

        @pl.when((i > 1) & (i < n - 1))
        def _():
            finish(i - 1)

        @pl.when(i >= keep)
        def _():
            swap(i - keep, 1).wait_send()

        product(i, 1, wu)

        @pl.when(i > 3)
        def _():
            stage(i - 3)

        retire(i - 1)

        @pl.when(i < n - 1)
        def _():
            ring(i, 0).wait_recv()
            ring(i, 1).wait_recv()
            pass_on(i + 1)
            scale_ring(i).wait_recv()
            scale_on(i + 1)

        @pl.when(i == n - 1)
        def _():
            finish(i - 1)

        @pl.when(i == 3)
        def _():
            load_d.wait()

        @pl.when(i > 2)
        def _():
            share(i - 2).wait_recv()

            @pl.when(i > 4)
            def _():
                sent(i - 4)

            down(i - 2)

    stage(n - 3)
    retire(n - 1)
    rv[0, col] = kept[...]
    finish(n - 1)
    again = (n - 1) // keep * keep
    share(again).wait_send()
    share(0).start()
    sent(n - 4)
    ring_free(n - 2)
    with jax.named_scope("share6"):
        share(n - 2).wait_recv()
    last(n - 2, lambda k: stage_part(n - 2, k))
    sent(n - 3)
    ring_free(n - 1)
    with jax.named_scope("share7"):
        share(n - 1).wait_recv()
    last(n - 1, lambda k: stage_part(n - 1, k))
    sent(n - 2)
    with jax.named_scope("share0"):
        share(0).wait_recv()
    last(0, final_part)

    sent(n - 1)

    @pl.loop(0, parts)
    def _(k):
        down_sib(0, k).wait_send()

    @pl.loop(n - keep, n)
    def _(s):
        swap(s, 0).wait_send()
        swap(s, 1).wait_send()

    for s in [0] + [s for s in range(n - keep, n) if s != again]:
        share(s).wait_send()
    scale_sib(n - 2).wait_send()
    scale_ring(n - 2).wait_send()
    scale_sib(n - 1).wait_send()


def kernels(rows, cols, tokens, norm_gain, gate_proj, up_proj, down_proj):
    n = rows // 2
    count, width = tokens.shape
    half = count // 2
    units = gate_proj.shape[1]
    lead = 256 if units % 256 == 0 else 128
    tile = units // 2 if units % 256 == 0 else lead
    parts = 4
    piece = width // parts
    vmem, hbm = pl.BlockSpec(memory_space=pltpu.VMEM), pl.BlockSpec(memory_space=pl.ANY)
    dma = pltpu.SemaphoreType.DMA
    return pl.pallas_call(
        functools.partial(fused_kernel, rows, cols, tile, lead),
        out_shape=jax.ShapeDtypeStruct(tokens.shape, BF),
        in_specs=[hbm, vmem, hbm, hbm, hbm],
        out_specs=vmem,
        scratch_shapes=[
            pltpu.VMEM(gate_proj.shape, BF),
            pltpu.VMEM(up_proj.shape, BF),
            pltpu.VMEM(down_proj.shape, BF),
            pltpu.VMEM((n, 2, 2, half, width), BF),
            pltpu.VMEM((4, 2, 2, 2 * half, units), BF),
            pltpu.VMEM((n, 2, 2 * half, units), BF),
            pltpu.VMEM((2, parts, 2, 2, half, piece), BF),
            pltpu.VMEM((2 * half, units), BF),
            pltpu.VMEM((2, half, 128), F32),
            pltpu.VMEM((half, 128), F32),
            pltpu.VMEM((n, 2, half, 128), F32),
            dma, dma((units // lead,)), dma, dma((2,)),
            dma((2, 2)), dma((n, 2)), dma((2,)), dma((n,)), dma((4, 3)), dma((4, 3)),
            dma((2, parts)), dma((3, parts)), dma((2, 2, parts)), dma((3, 2, parts)),
            dma((2, 2)), dma((n, 2)),
            pltpu.SemaphoreType.REGULAR((n, 3)),
        ],
        compiler_params=pltpu.CompilerParams(
            collective_id=0, has_side_effects=True, vmem_limit_bytes=67043328
        ),
    )(tokens, norm_gain.reshape(width // 128, 128), gate_proj, up_proj, down_proj)


def plain(rows, cols, tokens, norm_gain, gate_proj, up_proj, down_proj):
    gathered = lax.all_gather(tokens, "row", axis=0, tiled=True)
    widened = gathered.astype(jnp.float32)
    partial_squares = jnp.sum(widened * widened, axis=1)
    scaled = (widened * norm_gain.astype(jnp.float32)[None, :]).astype(jnp.bfloat16)
    gate_part = jnp.dot(scaled, gate_proj, preferred_element_type=jnp.float32)
    up_part = jnp.dot(scaled, up_proj, preferred_element_type=jnp.float32)
    gate_sum, up_sum, block_squares = (
        lax.psum_scatter(
            gate_part.astype(jnp.bfloat16), "col", scatter_dimension=0, tiled=True
        ).astype(jnp.float32),
        lax.psum_scatter(
            up_part.astype(jnp.bfloat16), "col", scatter_dimension=0, tiled=True
        ).astype(jnp.float32),
        lax.psum_scatter(
            partial_squares.astype(jnp.bfloat16), "col", scatter_dimension=0, tiled=True
        ).astype(jnp.float32),
    )
    row_scale = 1.0 / jnp.sqrt(block_squares / (tokens.shape[1] * cols) + floor_term)
    gate_value = row_scale[:, None] * gate_sum
    up_value = row_scale[:, None] * up_sum
    hidden = (jax.nn.silu(gate_value) * up_value).astype(jnp.bfloat16)
    partial_out = jnp.dot(
        lax.all_gather(hidden, "col", axis=0, tiled=True),
        down_proj,
        preferred_element_type=jnp.float32,
    )
    summed = lax.psum_scatter(
        partial_out.astype(jnp.bfloat16), "row", scatter_dimension=0, tiled=True
    ).astype(jnp.float32)
    return (tokens.astype(jnp.float32) + summed).astype(jnp.bfloat16)


def solution(mesh):
    rows, cols = mesh.shape["row"], mesh.shape["col"]
    body = kernels if cols == 2 and rows % 4 == 0 and rows >= 16 else plain
    in_specs = (P("row", "col"), P("col"), P("col", "row"), P("col", "row"), P("row", "col"))
    out_specs = P("row", "col")
    return jax.shard_map(
        functools.partial(body, rows, cols), mesh=mesh, in_specs=in_specs, out_specs=out_specs, check_vma=False
    )
```
